32 devices in a mesh: band: 16 (over z, x, core), lane: 2 (over y).
Axes of the slice: x: 2, y: 2, z: 4, core: 2. Of those that a mesh axis runs over, the one named last changes fastest.
Arguments:
- load_terms: float32 [1024, 128, 256], P('band', 'lane'), may hold values from -6 to 6
- start_values: float32 [1024, 128, 256], P('band', 'lane'), may hold values from -6 to 6
- reaction_rate: float32 [1024, 128, 256], P('band', 'lane'), may hold values from 0.1 to 0.9
Outputs:
- solution: float32 [1024, 128, 256], P('band', 'lane')
- remaining: float32 [1024, 128, 256], P('band', 'lane')
The draws below stay inside these ranges and needn't reach their ends.
All inputs are finite; a program needn't handle non-finite values.
Results may differ from the reference program's by a relative error of at most 0.0003.
Values sent between devices are 32-bit elements.
A program may use at most 128 MiB of HBM per device.

```python
import jax
import jax.numpy as jnp
from jax import lax

LAYERS = 256
RATIO = 2
BEFORE = 3
AFTER = 2
INNER = 13
GRID_Y = 1024
GRID_X = 128


def levels(key, dims, shards, smallest, high):
    factor_of, own = 1.0, jax.random.fold_in(key, 6)
    for axis_at, shards_of in shards:
        steps = jnp.exp(jax.random.uniform(jax.random.fold_in(own, axis_at), (shards_of,), jnp.float32, smallest / len(shards), high / len(shards)))
        factor_of = factor_of * jnp.repeat(steps, dims[axis_at] // shards_of).reshape([-1 if axis == axis_at else 1 for axis in range(len(dims))])
    return factor_of


def gaussian(own_key, shape, width, bound, cuts=(), kind=jnp.bfloat16):
    level = levels(own_key, shape, cuts, -0.22, 0.18) if cuts else 1.0
    entries = jax.random.normal(own_key, shape, jnp.float32) * width * level
    return jnp.minimum(jnp.maximum(entries, -bound), bound).astype(kind)


def setup_inputs(seed: int = 0) -> dict:
    seeds = jax.random.split(jax.random.key(seed), 4)
    load_terms = gaussian(seeds[0], (GRID_Y, GRID_X, LAYERS), 1.0, 6.0, ((0, 16), (1, 2)), jnp.float32)
    start_values = gaussian(seeds[1], (GRID_Y, GRID_X, LAYERS), 1.0, 6.0, ((0, 16), (1, 2)), jnp.float32)
    reaction_rate = jnp.clip(0.1 + 0.79999997 * jax.random.uniform(seeds[2], (GRID_Y, GRID_X, LAYERS), jnp.float32) ** levels(seeds[2], (GRID_Y, GRID_X, LAYERS), ((0, 16), (1, 2)), -0.2, 0.2), 0.1, 0.9)
    return dict(load_terms=load_terms, start_values=start_values, reaction_rate=reaction_rate)


def cross_sum(padded):
    inner_y, inner_x = padded.shape[0] - 2, padded.shape[1] - 2
    middle_rows = lax.slice_in_dim(padded, 1, 1 + inner_y, axis=0)
    middle_columns = lax.slice_in_dim(padded, 1, 1 + inner_x, axis=1)
    return (lax.slice_in_dim(middle_columns, 0, inner_y, axis=0) + lax.slice_in_dim(middle_columns, 2, 2 + inner_y, axis=0)
            + lax.slice_in_dim(middle_rows, 0, inner_x, axis=1) + lax.slice_in_dim(middle_rows, 2, 2 + inner_x, axis=1))


def smooth_step(padded, values, load, mass_here):
    return values + 0.8 * (load + cross_sum(padded) - (4.0 + mass_here) * values) / (4.0 + mass_here)


def block_means(values):
    cut = values.reshape(values.shape[0] // RATIO, RATIO, values.shape[1] // RATIO, RATIO, values.shape[2])
    return jnp.mean(cut, axis=(1, 3))


def spread_blocks(values):
    return jnp.repeat(jnp.repeat(values, RATIO, axis=0), RATIO, axis=1)


def reference(load_terms, start_values, reaction_rate):
    values = start_values
    for sweep in range(BEFORE):
        values = smooth_step(jnp.pad(values, ((1, 1), (1, 1), (0, 0)), mode="constant"), values, load_terms, reaction_rate)
    defect = load_terms + cross_sum(jnp.pad(values, ((1, 1), (1, 1), (0, 0)), mode="constant")) - (4.0 + reaction_rate) * values
    coarse_load, coarse_mass = block_means(defect) * RATIO, block_means(reaction_rate) * RATIO
    coarse_values = jnp.zeros_like(coarse_load)
    for sweep in range(INNER):
        coarse_values = smooth_step(jnp.pad(coarse_values, ((1, 1), (1, 1), (0, 0)), mode="constant"), coarse_values, coarse_load, coarse_mass)
    values = values + spread_blocks(coarse_values)
    for sweep in range(AFTER):
        values = smooth_step(jnp.pad(values, ((1, 1), (1, 1), (0, 0)), mode="constant"), values, load_terms, reaction_rate)
    solution = values
    remaining = load_terms + cross_sum(jnp.pad(solution, ((1, 1), (1, 1), (0, 0)), mode="constant")) - (4.0 + reaction_rate) * solution
    return solution, remaining
```

```python
import functools

import jax
import jax.numpy as jnp
from jax import lax
from jax.experimental import pallas as pl
from jax.experimental.pallas import tpu as pltpu
from jax.sharding import PartitionSpec as P

BEFORE = 3
AFTER = 2
INNER = 13
OMEGA = 0.8
LANES = 128
DEPTH = 4
PAD = 8
CX = 16
MESH = pl.DeviceIdType.MESH


def kernel(
    bands, lanes, load_hbm, start_hbm, rate_hbm, sol_hbm, rem_hbm,
    u, f, w, diag, pair, cu, cl, cw, col_out, col_in, ccol_out, ccol_in, crow_in,
    in_sem, out_sem, send_sem, recv_sem, csend_sem, crecv_sem,
):
    ny, nx = f.shape[1], f.shape[2]
    my, mx = ny // 2, nx // 2
    chunks = f.shape[0]
    wide = mx + 2 * PAD
    band, lane = lax.axis_index("band"), lax.axis_index("lane")
    near = (
        (band > 0, {"band": band - 1}),
        (band < bands - 1, {"band": band + 1}),
        (lane > 0, {"lane": lane - 1}),
        (lane < lanes - 1, {"lane": lane + 1}),
    )
    fine_x = pl.ds(PAD, nx)

    def loads(c):
        part = pl.ds(c * LANES, LANES)
        return (
            pltpu.make_async_copy(start_hbm.at[:, :, part], u.at[0, c, pl.ds(1, ny), fine_x], in_sem.at[c, 0]),
            pltpu.make_async_copy(rate_hbm.at[:, :, part], diag.at[c], in_sem.at[c, 1]),
            pltpu.make_async_copy(load_hbm.at[:, :, part], f.at[c], in_sem.at[c, 2]),
        )

    def stores(c):
        part = pl.ds(c * LANES, LANES)
        final = (BEFORE + 1 + AFTER) % 2
        return (
            pltpu.make_async_copy(u.at[final, c, pl.ds(1, ny), fine_x], sol_hbm.at[:, :, part], out_sem.at[c, 0]),
            pltpu.make_async_copy(w.at[c], rem_hbm.at[:, :, part], out_sem.at[c, 1]),
        )

    for at in (0, 1, 2):
        for c in range(chunks):
            loads(c)[at].start()

    barrier = pltpu.get_barrier_semaphore()
    count = 0
    for there, device in near:
        count = count + there.astype(jnp.int32)

    zero_col = jnp.zeros((PAD, LANES), jnp.float32)
    for slot in range(2):
        for c in range(chunks):
            for y in (0, ny + 1):
                u[slot, c, y] = jnp.zeros(u.shape[3:], jnp.float32)

    @pl.loop(1, ny + 1)
    def _(y):
        for slot in range(2):
            for c in range(chunks):
                u[slot, c, y, 0:PAD, :] = zero_col
                u[slot, c, y, PAD + nx : 2 * PAD + nx, :] = zero_col

    @pl.loop(0, my + 2 * DEPTH)
    def _(y):
        zero_row = jnp.zeros(cu.shape[3:], jnp.float32)
        for c in range(chunks):
            cu[0, c, y] = zero_row
            cu[1, c, y] = zero_row
            cl[c, y] = zero_row
            cw[c, y] = zero_row

    for there, device in near:

        @pl.when(there)
        def _():
            pl.semaphore_signal(barrier, inc=1, device_id=device, device_id_type=MESH)

    pl.semaphore_wait(barrier, count)

    def fine_copy(k, c, side, device):
        p, o = k % 2, side ^ 1
        if side < 2:
            src = u.at[p, c, 1 if side == 0 else ny, fine_x]
            dst = u.at[p, c, ny + 1 if side == 0 else 0, fine_x]
        else:
            src = col_out.at[p, c, side - 2]
            dst = col_in.at[p, c, o - 2]
        return pltpu.make_async_remote_copy(
            src_ref=src, dst_ref=dst, send_sem=send_sem.at[p, c, side], recv_sem=recv_sem.at[p, c, o],
            device_id=device, device_id_type=MESH,
        )

    def send_fine(k, c):
        p = k % 2

        @pl.loop(0, ny, unroll=8)
        def _(y):
            col_out[p, c, 0, pl.ds(y, 1), :] = u[p, c, 1 + y, PAD : PAD + 1, :]
            col_out[p, c, 1, pl.ds(y, 1), :] = u[p, c, 1 + y, PAD + nx - 1 : PAD + nx, :]

        for side in (2, 3, 0, 1):
            there, device = near[side]

            @pl.when(there)
            def _():
                fine_copy(k, c, side, device).start()

    def wait_fine(k, c):
        p = k % 2
        for side in (0, 1, 2, 3):
            there, device = near[side]

            @pl.when(there)
            def _():
                fine_copy(k, c, side, device).wait_send()
                fine_copy(k, c, side ^ 1, device).wait_recv()
                if side >= 2:
                    at = PAD - 1 if side == 2 else PAD + nx

                    @pl.loop(0, ny, unroll=8)
                    def _(y):
                        u[p, c, 1 + y, at : at + 1, :] = col_in[p, c, side - 2, pl.ds(y, 1), :]

    def cross(ref, y, x, rows):
        middle = [ref[y + i - 1, pl.ds(x, 8), :] for i in range(rows + 2)]
        return [
            (
                middle[i + 1],
                (middle[i] + middle[i + 2])
                + (ref[y + i, pl.ds(x - 1, 8), :] + ref[y + i, pl.ds(x + 1, 8), :]),
            )
            for i in range(rows)
        ]

    def sweep_fine(k, c):
        src, dst, ff, ww = u.at[k % 2, c], u.at[(k + 1) % 2, c], f.at[c], w.at[c]
        rows = 4

        @pl.loop(0, ny // rows)
        def _(g):
            y = g * rows
            for x in range(0, nx, 8):
                for i, (here, total) in enumerate(cross(src, y + 1, PAD + x, rows)):
                    new = (1.0 - OMEGA) * here + ww[y + i, pl.ds(x, 8), :] * (ff[y + i, pl.ds(x, 8), :] + total)
                    dst[y + 1 + i, pl.ds(PAD + x, 8), :] = new

    def halve(slot):
        return pair[slot, pl.ds(0, mx, stride=2), :] + pair[slot, pl.ds(1, mx, stride=2), :]

    def prepare(c):
        @pl.loop(0, my)
        def _(j):
            y = 2 * j
            for x in range(0, nx, 8):
                part = pl.ds(x, 8)
                m0, m1 = diag[c, y, part, :], diag[c, y + 1, part, :]
                pair[c, part, :] = m0 + m1
                d0, d1 = 4.0 + m0, 4.0 + m1
                diag[c, y, part, :] = d0
                diag[c, y + 1, part, :] = d1
                w[c, y, part, :] = OMEGA / d0
                w[c, y + 1, part, :] = OMEGA / d1
            cw[c, DEPTH + j, CX : CX + mx, :] = OMEGA / (4.0 + 0.5 * halve(c))

    def restrict(k, c):
        src = u.at[k % 2, c]

        @pl.loop(0, my)
        def _(j):
            y = 2 * j
            for x in range(0, nx, 8):
                part = pl.ds(x, 8)
                both = [
                    f[c, y + i, part, :] + total - diag[c, y + i, part, :] * here
                    for i, (here, total) in enumerate(cross(src, y + 1, PAD + x, 2))
                ]
                pair[c, part, :] = both[0] + both[1]
            cl[c, DEPTH + j, CX : CX + mx, :] = 0.5 * halve(c)

    def coarse_ref(slot, c):
        return (cw.at[c], cl.at[c])[slot] if slot < 2 else cu.at[0, c]

    def coarse_copy(slot, c, side, device):
        o = side ^ 1
        if side < 2:
            src = coarse_ref(slot, c).at[pl.ds(DEPTH if side == 0 else my, DEPTH), pl.ds(CX - PAD, wide)]
            dst = crow_in.at[slot, c, o]
        else:
            src = ccol_out.at[slot, c, side - 2]
            dst = ccol_in.at[slot, c, o - 2]
        return pltpu.make_async_remote_copy(
            src_ref=src, dst_ref=dst, send_sem=csend_sem.at[slot, c, side], recv_sem=crecv_sem.at[slot, c, o],
            device_id=device, device_id_type=MESH,
        )

    def send_columns(slot, c):
        ref = coarse_ref(slot, c)

        @pl.loop(0, my, unroll=8)
        def _(y):
            ccol_out[slot, c, 0, pl.ds(y * DEPTH, DEPTH), :] = ref[DEPTH + y, CX : CX + DEPTH, :]
            ccol_out[slot, c, 1, pl.ds(y * DEPTH, DEPTH), :] = ref[DEPTH + y, CX + mx - DEPTH : CX + mx, :]

        for side in (2, 3):
            there, device = near[side]

            @pl.when(there)
            def _():
                coarse_copy(slot, c, side, device).start()

    def columns_then_rows(slot, c):
        ref = coarse_ref(slot, c)
        for side in (2, 3):
            there, device = near[side]

            @pl.when(there)
            def _():
                coarse_copy(slot, c, side, device).wait_send()
                coarse_copy(slot, c, side ^ 1, device).wait_recv()
                at = CX - DEPTH if side == 2 else CX + mx

                @pl.loop(0, my, unroll=8)
                def _(y):
                    ref[DEPTH + y, at : at + DEPTH, :] = ccol_in[slot, c, side - 2, pl.ds(y * DEPTH, DEPTH), :]

        for side in (0, 1):
            there, device = near[side]

            @pl.when(there)
            def _():
                coarse_copy(slot, c, side, device).start()

    def wait_rows(slot, c):
        ref = coarse_ref(slot, c)
        for side in (0, 1):
            there, device = near[side]
            at = 0 if side == 0 else DEPTH + my

            @pl.when(there)
            def _():
                coarse_copy(slot, c, side, device).wait_send()
                coarse_copy(slot, c, side ^ 1, device).wait_recv()
                for i in range(DEPTH):
                    ref[at + i, pl.ds(CX - PAD, wide), :] = crow_in[slot, c, side, i]

    def sweep_coarse(s, c):
        src, dst, ff, ww = cu.at[s % 2, c], cu.at[(s + 1) % 2, c], cl.at[c], cw.at[c]
        rows = 2
        first, number = s + 1, my + 2 * DEPTH - 2 * (s + 1)

        @pl.loop(0, number // rows)
        def _(g):
            y = first + g * rows
            for x in range(CX - PAD, CX - PAD + wide, 8):
                for i, (here, total) in enumerate(cross(src, y, x, rows)):
                    part = pl.ds(x, 8)
                    dst[y + i, part, :] = (1.0 - OMEGA) * here + ww[y + i, part, :] * (ff[y + i, part, :] + total)

    def first_coarse(c):
        @pl.loop(0, my + 2 * DEPTH)
        def _(y):
            part = pl.ds(CX - PAD, wide)
            cu[0, c, y, part, :] = cw[c, y, part, :] * cl[c, y, part, :]

    def correct(k, c):
        @pl.loop(0, my)
        def _(j):
            add = cu[0, c, DEPTH + j, CX : CX + mx, :]
            for i in range(2):
                for odd in range(2):
                    part = pl.ds(PAD + odd, mx, stride=2)
                    u[(k + 1) % 2, c, 1 + 2 * j + i, part, :] = u[k % 2, c, 1 + 2 * j + i, part, :] + add

    def leave(k, c):
        src = u.at[k % 2, c]
        rows = 4

        @pl.loop(0, ny // rows)
        def _(g):
            y = g * rows
            for x in range(0, nx, 8):
                part = pl.ds(x, 8)
                for i, (here, total) in enumerate(cross(src, y + 1, PAD + x, rows)):
                    w[c, y + i, part, :] = f[c, y + i, part, :] + total - diag[c, y + i, part, :] * here

    both = range(chunks)
    for c in both:
        loads(c)[0].wait()
        send_fine(0, c)
    for c in both:
        loads(c)[1].wait()
        prepare(c)
        send_columns(0, c)
    for c in both:
        loads(c)[2].wait()
    k = 0
    for sweep in range(BEFORE):
        for c in both:
            wait_fine(k, c)
            sweep_fine(k, c)
            send_fine(k + 1, c)
            if sweep == 0:
                columns_then_rows(0, c)
            if sweep == 1:
                wait_rows(0, c)
        k += 1
    for c in both:
        wait_fine(k, c)
        restrict(k, c)
        send_columns(1, c)
    for c in both:
        columns_then_rows(1, c)
    rounds = (INNER - 1) // DEPTH
    for turn in range(rounds):
        for c in both:
            wait_rows(1 + turn, c)
            if turn == 0:
                first_coarse(c)
            for s in range(DEPTH):
                sweep_coarse(s, c)
            if turn < rounds - 1:
                send_columns(2 + turn, c)
            else:
                correct(k, c)
                send_fine(k + 1, c)
        if turn < rounds - 1:
            for c in both:
                columns_then_rows(2 + turn, c)
    k += 1
    for sweep in range(AFTER):
        for c in both:
            wait_fine(k, c)
            sweep_fine(k, c)
            send_fine(k + 1, c)
            if sweep == AFTER - 1:
                stores(c)[0].start()
        k += 1
    for c in both:
        wait_fine(k, c)
        leave(k, c)
        stores(c)[1].start()
    for c in both:
        for copy in stores(c):
            copy.wait()


def solution(mesh):
    bands, lanes = mesh.shape["band"], mesh.shape["lane"]

    def on_device(load_terms, start_values, reaction_rate):
        ny, nx, layers = load_terms.shape
        chunks = layers // LANES
        my, mx = ny // 2, nx // 2
        slots = 1 + (INNER - 1) // DEPTH
        f32 = jnp.float32
        vmem = lambda *shape: pltpu.VMEM(shape + (LANES,), f32)
        dma = lambda *shape: pltpu.SemaphoreType.DMA(shape)
        return pl.pallas_call(
            functools.partial(kernel, bands, lanes),
            out_shape=[jax.ShapeDtypeStruct(load_terms.shape, f32)] * 2,
            in_specs=[pl.BlockSpec(memory_space=pl.ANY)] * 3,
            out_specs=[pl.BlockSpec(memory_space=pl.ANY)] * 2,
            scratch_shapes=[
                vmem(2, chunks, ny + 2, nx + 2 * PAD),
                vmem(chunks, ny, nx),
                vmem(chunks, ny, nx),
                vmem(chunks, ny, nx),
                vmem(chunks, nx),
                vmem(2, chunks, my + 2 * DEPTH, mx + 2 * CX),
                vmem(chunks, my + 2 * DEPTH, mx + 2 * CX),
                vmem(chunks, my + 2 * DEPTH, mx + 2 * CX),
                vmem(2, chunks, 2, ny),
                vmem(2, chunks, 2, ny),
                vmem(slots, chunks, 2, my * DEPTH),
                vmem(slots, chunks, 2, my * DEPTH),
                vmem(slots, chunks, 2, DEPTH, mx + 2 * PAD),
                dma(chunks, 3),
                dma(chunks, 2),
                dma(2, chunks, 4),
                dma(2, chunks, 4),
                dma(slots, chunks, 4),
                dma(slots, chunks, 4),
            ],
            compiler_params=pltpu.CompilerParams(
                collective_id=0, has_side_effects=True, vmem_limit_bytes=60 * 1024 * 1024
            ),
        )(load_terms, start_values, reaction_rate)

    placed = P("band", "lane", None)
    return jax.shard_map(
        on_device, mesh=mesh, in_specs=(placed,) * 3, out_specs=(placed, placed), check_vma=False
    )
```
